32 devices in a mesh: ha: 2 (over x), vert: 16 (over z, y, core).
Axes of the slice: x: 2, y: 2, z: 4, core: 2. Of those that a mesh axis runs over, the one named last changes fastest.
Arguments:
- hidden: bfloat16 [128, 16384], P('vert', 'ha'), may hold values from -6 to 6
- norm_gain: float32 [16384], P('ha'), may hold values from 0.25 to 1.75
- head_weight: bfloat16 [16384, 32064], P('ha', 'vert'), may hold values from -0.046875 to 0.046875
- targets: int32 [128], replicated, may hold values from 0 to 32063
Outputs:
- log_probs: float32 [128, 32064], P('ha', 'vert')
- target_logprob: float32 [128], P('ha')
The draws below stay inside these ranges and needn't reach their ends.
Inputs may be any that keep to these rules, and one draw needn't show every extreme that they name: `targets`: every next token id lies in 0 to 32063.
All inputs are finite; a program needn't handle non-finite values.
Results may differ from the reference program's by a relative error of at most 0.0015.
Values may be sent and summed in bfloat16 or wider, within the bound.
A program may use at most 64 MiB of HBM per device.

```python
import jax
import jax.numpy as jnp
from jax import lax

D = 16384
BATCH = 128
VOCAB = 32064


def plant(array, key, low, high):
    longest = array.shape.index(max(array.shape))
    spots = []
    for shift in (0, 1):
        where = [jax.random.randint(jax.random.fold_in(key, axis), (), 0, length) for axis, length in enumerate(array.shape)]
        where[longest] = (where[longest] + shift) % array.shape[longest]
        spots.append(tuple(where))
    return array.at[spots[0]].set(low).at[spots[1]].set(high)


def levels(stream_key, extent, cuts, smallest, high):
    factor_of, own = 1.0, jax.random.fold_in(stream_key, 6)
    for axis_at, parts in cuts:
        draws = jnp.exp(jax.random.uniform(jax.random.fold_in(own, axis_at), (parts,), jnp.float32, smallest / len(cuts), high / len(cuts)))
        factor_of = factor_of * jnp.repeat(draws, extent[axis_at] // parts).reshape([-1 if axis == axis_at else 1 for axis in range(len(extent))])
    return factor_of


def bell_draw(own_key, shape, width, reach, pieces=(), kind=jnp.bfloat16):
    drawn = width * jax.random.normal(own_key, shape, jnp.float32)
    if pieces:
        drawn = drawn * levels(own_key, shape, pieces, -0.22, 0.18)
    return jnp.clip(drawn, -reach, reach).astype(kind)


def setup_inputs(seed: int = 0) -> dict:
    keys = jax.random.split(jax.random.key(seed), 5)
    return {
        "hidden": bell_draw(keys[0], (BATCH, D), 1.0, 6.0, ((0, 16), (1, 2))),
        "norm_gain": jnp.clip(1.0 + 0.15 * jax.random.normal(keys[1], (D,), jnp.float32), 0.25, 1.75),
        "head_weight": bell_draw(keys[2], (D, VOCAB), D ** -0.5, 0.046875, ((0, 2), (1, 16))),
        "targets": plant(jax.random.randint(keys[3], (BATCH,), 0, VOCAB), jax.random.fold_in(keys[3], 1), 0, VOCAB - 1).astype(jnp.int32),
    }


def reference(hidden, norm_gain, head_weight, targets):
    widened = hidden.astype(jnp.float32)
    squares = lax.optimization_barrier(jnp.sum(widened * widened, axis=1))
    inverse = lax.rsqrt(squares / D + 1e-05)
    scaled = (widened * norm_gain[None, :]).astype(jnp.bfloat16)
    logits = jnp.dot(scaled, head_weight, preferred_element_type=jnp.float32) * inverse[:, None]
    largest = lax.optimization_barrier(jnp.max(logits, axis=1))
    log_total = largest + jnp.log(lax.optimization_barrier(jnp.sum(jnp.exp(logits - largest[:, None]), axis=1)))
    log_probs = logits - log_total[:, None]
    picked = jnp.take_along_axis(log_probs, targets.astype(jnp.int32)[:, None], axis=1)[:, 0]
    return (log_probs, picked)
```

```python
import functools

import jax
import jax.numpy as jnp
from jax import lax
from jax.experimental import pallas as pl
from jax.experimental.pallas import tpu as pltpu
from jax.sharding import PartitionSpec as P

D = 16384


def combined_all(part, axis, combine):
    gathered = jax.tree.map(lambda a: lax.all_gather(a, axis), part)

    def take(source):
        return jax.tree.map(lambda a: lax.dynamic_index_in_dim(a, source, 0, False), gathered)

    return lax.fori_loop(
        1, lax.axis_size(axis), lambda source, state: combine(state, take(source)), take(0)
    )


def combine(earlier, later_one):
    largest = jnp.maximum(earlier[0], later_one[0])
    expsum = earlier[1] * jnp.exp(earlier[0] - largest) + later_one[1] * jnp.exp(
        later_one[0] - largest
    )
    return (largest, expsum, earlier[2] + later_one[2])


def shards(hidden, norm_gain, head_weight, targets):
    vocab_width = head_weight.shape[1]
    vocab_start = lax.axis_index("vert") * vocab_width
    ha_count = lax.axis_size("ha")
    batch_total = hidden.shape[0] * lax.axis_size("vert")
    own_rows = batch_total // ha_count

    def partial_terms(block_rows):
        widened = block_rows.astype(jnp.float32)
        scaled = (widened * norm_gain[None, :]).astype(jnp.bfloat16)
        product = jnp.dot(scaled, head_weight, preferred_element_type=jnp.float32)
        squares = jnp.sum(widened * widened, axis=1, keepdims=True)
        return jnp.concatenate([product, squares], axis=1)

    def finish(summed, row_targets):
        unscaled = summed[:, :vocab_width]
        inverse = lax.rsqrt(summed[:, vocab_width:] / D + 1e-05)
        logits = unscaled * inverse
        local_max = jnp.max(logits, axis=1)
        local_sum = jnp.sum(jnp.exp(logits - local_max[:, None]), axis=1)
        columns = vocab_start + jnp.arange(vocab_width, dtype=jnp.int32)
        matches = row_targets[:, None] == columns[None, :]
        local_target = jnp.sum(jnp.where(matches, logits, 0.0), axis=1)
        largest, expsum, target_sum = combined_all(
            (local_max, local_sum, local_target), "vert", combine
        )
        log_total = largest + jnp.log(expsum)
        return (logits - log_total[:, None], target_sum - log_total)

    first_row = lax.axis_index("ha") * own_rows
    gathered = lax.all_gather(hidden, "vert", axis=0, tiled=True)
    summed = lax.psum_scatter(
        partial_terms(lax.slice_in_dim(gathered, 0, own_rows * lax.axis_size("ha"), axis=0)).astype(
            jnp.bfloat16
        ),
        "ha",
        scatter_dimension=0,
        tiled=True,
    ).astype(jnp.float32)
    row_targets = lax.dynamic_slice_in_dim(targets, first_row, own_rows, 0)
    log_probs, picked = finish(summed, row_targets)
    return (log_probs, picked)


MESH = pl.DeviceIdType.MESH
CORES = 2
INNER = 2
LANES = 128


def tiles_of(width, tile):
    return [(start, min(tile, width - start)) for start in range(0, width, tile)]


def kernel(
    sizes, hidden_ref, gain_ref, weight_ref, targets_ref, out_ref, picked_ref,
    gathered, weight, total, turned, squares, stats, square_in, square_out, *rest
):
    outer, chunks, depth, batch, own_rows, tiles = sizes
    count = len(tiles)
    outgoing, incoming = rest[:count], rest[count : 2 * count]
    (own_sem, weight_sem, z_send, z_recv, y_send, y_recv, d_send, d_recv,
     x_send, x_recv, q_send, q_recv, s_send, s_recv) = rest[2 * count :]
    ha = lax.axis_index("ha")
    me = lax.axis_index("vert")
    vert = outer * INNER * CORES
    z, y, c = me // (INNER * CORES), (me // CORES) % INNER, me % CORES

    def at(zz, yy, cc):
        return (ha, (zz * INNER + yy) * CORES + cc)

    across = (1 - ha, me)
    beside = at(z, 1 - y, c)
    sibling = at(z, y, 1 - c)

    own_copies = [
        pltpu.make_async_copy(
            hidden_ref.at[:, pl.ds(k * depth, depth)], gathered.at[k, z, y, c], own_sem.at[k]
        )
        for k in range(chunks)
    ]
    for copy in own_copies:
        copy.start()
    weight_copies = [
        pltpu.make_async_copy(
            weight_ref.at[:, pl.ds(k * depth, depth)], weight.at[k], weight_sem.at[k]
        )
        for k in range(chunks)
    ]
    for copy in weight_copies:
        copy.start()

    barrier = pltpu.get_barrier_semaphore()
    for step in range(1, vert):
        pl.semaphore_signal(
            barrier, inc=1, device_id=(ha, (me + step) % vert), device_id_type=MESH
        )
    pl.semaphore_signal(barrier, inc=1, device_id=across, device_id_type=MESH)
    pl.semaphore_wait(barrier, vert)

    def remote(src, dst, send, recv, device):
        return pltpu.make_async_remote_copy(
            src_ref=src, dst_ref=dst, send_sem=send, recv_sem=recv,
            device_id=device, device_id_type=MESH,
        )

    for k in range(chunks):
        own_copies[k].wait()
        mine = gathered.at[k, z, y, c]
        for step in range(1, outer):
            remote(mine, mine, z_send.at[k], z_recv.at[k], at((z + step) % outer, y, c)).start()
        remote(mine, mine, y_send.at[k], y_recv.at[k], beside).start()

    total[...] = jnp.zeros_like(total)
    squares[...] = jnp.zeros_like(squares)

    def three(k, send, recv, device):
        block = gathered.at[k, pl.ds(0, outer - 1), 0, 0]
        return remote(block, block, send.at[k], recv.at[k], device)

    def four(k, send, recv, device):
        block = gathered.at[k, :, 0, 0]
        return remote(block, block, send.at[k], recv.at[k], device)

    def eight(k, send, recv, device):
        block = gathered.at[k, :, :, 0]
        return remote(block, block, send.at[k], recv.at[k], device)

    def stage_a(k):
        three(k, z_send, z_recv, beside).wait_recv()
        for step in range(1, outer):
            piece = gathered.at[k, (z + step) % outer, y, c]
            remote(piece, piece, y_send.at[k], y_recv.at[k], beside).start()
        column = gathered.at[k, :, y, c]
        remote(column, column, d_send.at[k], d_recv.at[k], sibling).start()

    def stage_b(k):
        four(k, y_send, y_recv, beside).wait_recv()
        column = gathered.at[k, :, 1 - y, c]
        remote(column, column, d_send.at[k], d_recv.at[k], sibling).start()

    def stage_c(k):
        eight(k, d_send, d_recv, sibling).wait_recv()
        pltpu.make_async_copy(
            weight_ref.at[:, pl.ds(pl.multiple_of(k * depth, depth), depth)],
            weight.at[k], weight_sem.at[k],
        ).wait()
        widened = gathered[k].astype(jnp.float32).reshape(batch, depth)
        squares[...] += sum(
            widened[:, lane : lane + LANES] * widened[:, lane : lane + LANES]
            for lane in range(0, depth, LANES)
        )
        gain = gain_ref[k]
        return (widened * gain).astype(jnp.bfloat16)

    def product(k, scaled, tile):
        start, width = tile
        return lax.dot_general(
            weight[k, pl.ds(start, width), :], scaled, (((1,), (1,)), ((), ())),
            preferred_element_type=jnp.float32,
        )

    stage_a(0)
    stage_a(1)
    stage_b(0)

    def body(k, carry):
        @pl.when(k + 2 < chunks)
        def _():
            stage_a(k + 2)

        stage_b(k + 1)
        scaled = stage_c(k)
        for tile in tiles:
            total[pl.ds(*tile), :] += product(k, scaled, tile)
        return carry

    lax.fori_loop(0, chunks - 1, body, 0)

    last = chunks - 1
    scaled = stage_c(last)
    kept = pl.ds(pl.multiple_of(ha * own_rows, own_rows), own_rows)
    given = pl.ds(pl.multiple_of((1 - ha) * own_rows, own_rows), own_rows)
    square_out[...] = squares[given, :]
    square_copy = remote(square_out, square_in, q_send.at[0], q_recv.at[0], across)
    square_copy.start()
    x_copies = []
    for j, tile in enumerate(tiles):
        total[pl.ds(*tile), :] += product(last, scaled, tile)
        padded = pl.ds(tile[0], TILE)
        turned[:, padded] = jnp.transpose(total[padded, :])
        outgoing[j][...] = turned[given, pl.ds(*tile)].astype(jnp.bfloat16)
        copy = remote(outgoing[j], incoming[j], x_send.at[j], x_recv.at[j], across)
        copy.start()
        x_copies.append(copy)

    square_copy.wait_recv()
    summed = jnp.sum(squares[kept, :] + square_in[...], axis=1, keepdims=True)
    inverse = lax.rsqrt(summed / D + 1e-05)
    largest = None
    for j, tile in enumerate(tiles):
        x_copies[j].wait_recv()
        logits = (turned[kept, pl.ds(*tile)] + incoming[j][...].astype(jnp.float32)) * inverse
        out_ref[:, pl.ds(*tile)] = logits
        top = jnp.max(logits, axis=1, keepdims=True)
        largest = top if largest is None else jnp.maximum(largest, top)
    wanted = jnp.transpose(
        jnp.broadcast_to(targets_ref[pl.ds(ha, 1), :].astype(jnp.float32), (LANES, LANES))
    )[:own_rows, 0:1].astype(jnp.int32)
    base = me * out_ref.shape[1]
    expsum = jnp.zeros_like(largest)
    target_sum = jnp.zeros_like(largest)
    for start, width in tiles:
        logits = out_ref[:, pl.ds(start, width)]
        expsum += jnp.sum(jnp.exp(logits - largest), axis=1, keepdims=True)
        columns = base + start + lax.broadcasted_iota(jnp.int32, logits.shape, 1)
        target_sum += jnp.sum(
            jnp.where(columns == wanted, logits, 0.0), axis=1, keepdims=True
        )
    lane = lax.broadcasted_iota(jnp.int32, (own_rows, LANES), 1)
    packed = jnp.where(lane == 0, largest, jnp.where(lane == 1, expsum, target_sum))
    packed = jnp.concatenate([packed] * (LANES // own_rows), axis=0)
    stats[me] = jnp.transpose(packed)[0:8, :]
    copies = [
        remote(stats.at[me], stats.at[me], s_send, s_recv, (ha, (me + step) % vert))
        for step in range(1, vert)
    ]
    for copy in copies:
        copy.start()
    others = stats.at[pl.ds(0, vert - 1)]
    remote(others, others, s_send, s_recv, sibling).wait_recv()
    tops = stats[:, 0, :]
    overall = jnp.max(tops, axis=0, keepdims=True)
    sums = jnp.sum(jnp.exp(tops - overall) * stats[:, 1, :], axis=0, keepdims=True)
    log_total = overall + jnp.log(sums)
    picked_ref[...] = jnp.sum(stats[:, 2, :], axis=0, keepdims=True) - log_total
    column = jnp.transpose(jnp.broadcast_to(log_total, (LANES, LANES)))[:own_rows, 0:1]
    for tile in tiles:
        out_ref[:, pl.ds(*tile)] = out_ref[:, pl.ds(*tile)] - column

    remote(others, others, s_send, s_recv, sibling).wait_send()
    square_copy.wait_send()
    for copy in x_copies:
        copy.wait_send()

    def drain(k, carry):
        three(k, z_send, z_recv, beside).wait_send()
        four(k, y_send, y_recv, beside).wait_send()
        eight(k, d_send, d_recv, sibling).wait_send()
        return carry

    lax.fori_loop(0, chunks, drain, 0)


def fused(hidden, norm_gain, head_weight, targets):
    rows, features = hidden.shape
    vocab_width = head_weight.shape[1]
    vert = lax.axis_size("vert")
    outer = vert // (INNER * CORES)
    batch = rows * vert
    own_rows = batch // lax.axis_size("ha")
    chunks = CHUNKS
    depth = features // chunks
    tiles = tiles_of(vocab_width, TILE)
    dma = pltpu.SemaphoreType.DMA
    any_space = pl.BlockSpec(memory_space=pl.ANY)
    vmem = pl.BlockSpec(memory_space=pltpu.VMEM)
    targets = targets.reshape(2, own_rows)
    targets = jnp.concatenate([targets] * (LANES // own_rows), axis=1)
    log_probs, picked = pl.pallas_call(
        functools.partial(kernel, (outer, chunks, depth, batch, own_rows, tiles)),
        out_shape=(
            jax.ShapeDtypeStruct((own_rows, vocab_width), jnp.float32),
            jax.ShapeDtypeStruct((1, LANES), jnp.float32),
        ),
        in_specs=[any_space, vmem, any_space, vmem],
        out_specs=(vmem, vmem),
        scratch_shapes=[
            pltpu.VMEM((chunks, outer, INNER, CORES, rows, depth), jnp.bfloat16),
            pltpu.VMEM((chunks, vocab_width, depth), jnp.bfloat16),
            pltpu.VMEM((TILE * len(tiles), batch), jnp.float32),
            pltpu.VMEM((batch, TILE * len(tiles)), jnp.float32),
            pltpu.VMEM((batch, LANES), jnp.float32),
            pltpu.VMEM((vert, 8, LANES), jnp.float32),
            pltpu.VMEM((own_rows, LANES), jnp.float32),
            pltpu.VMEM((own_rows, LANES), jnp.float32),
        ]
        + [pltpu.VMEM((own_rows, width), jnp.bfloat16) for _, width in tiles] * 2
        + [dma((chunks,))] * 8
        + [dma((len(tiles),))] * 2
        + [dma((1,))] * 2
        + [dma(())] * 2,
        compiler_params=pltpu.CompilerParams(
            collective_id=0, has_side_effects=True, vmem_limit_bytes=60 * 1024 * 1024
        ),
        name="head",
    )(hidden, norm_gain.reshape(chunks, 1, depth), head_weight.T, targets)
    return log_probs, picked[0, :own_rows]


def local(hidden, norm_gain, head_weight, targets):
    rows, features = hidden.shape
    vert, ha = lax.axis_size("vert"), lax.axis_size("ha")
    own_rows = rows * vert // ha
    fits = (
        rows == 8
        and ha == 2
        and LANES % own_rows == 0
        and vert % (INNER * CORES) == 0
        and vert > INNER * CORES
        and features % (CHUNKS * LANES) == 0
        and head_weight.size * 2 <= 40 * 2**20
    )
    return (fused if fits else shards)(hidden, norm_gain, head_weight, targets)


CHUNKS = 8
TILE = 512


def solution(mesh):
    placed = (P("vert", "ha"), P("ha"), P("ha", "vert"), P())
    return jax.shard_map(
        local, mesh=mesh, in_specs=placed, out_specs=(P("ha", "vert"), P("ha")), check_vma=False
    )
```

```python
import functools

import jax
import jax.numpy as jnp
from jax import lax
from jax.experimental import pallas as pl
from jax.experimental.pallas import tpu as pltpu
from jax.sharding import PartitionSpec as P

D = 16384


def combined_all(part, axis, combine):
    gathered = jax.tree.map(lambda a: lax.all_gather(a, axis), part)

    def take(source):
        return jax.tree.map(lambda a: lax.dynamic_index_in_dim(a, source, 0, False), gathered)

    return lax.fori_loop(
        1, lax.axis_size(axis), lambda source, state: combine(state, take(source)), take(0)
    )


def combine(earlier, later_one):
    largest = jnp.maximum(earlier[0], later_one[0])
    expsum = earlier[1] * jnp.exp(earlier[0] - largest) + later_one[1] * jnp.exp(
        later_one[0] - largest
    )
    return (largest, expsum, earlier[2] + later_one[2])


def shards(hidden, norm_gain, head_weight, targets):
    vocab_width = head_weight.shape[1]
    vocab_start = lax.axis_index("vert") * vocab_width
    ha_count = lax.axis_size("ha")
    batch_total = hidden.shape[0] * lax.axis_size("vert")
    own_rows = batch_total // ha_count

    def partial_terms(block_rows):
        widened = block_rows.astype(jnp.float32)
        scaled = (widened * norm_gain[None, :]).astype(jnp.bfloat16)
        product = jnp.dot(scaled, head_weight, preferred_element_type=jnp.float32)
        squares = jnp.sum(widened * widened, axis=1, keepdims=True)
        return jnp.concatenate([product, squares], axis=1)

    def finish(summed, row_targets):
        unscaled = summed[:, :vocab_width]
        inverse = lax.rsqrt(summed[:, vocab_width:] / D + 1e-05)
        logits = unscaled * inverse
        local_max = jnp.max(logits, axis=1)
        local_sum = jnp.sum(jnp.exp(logits - local_max[:, None]), axis=1)
        columns = vocab_start + jnp.arange(vocab_width, dtype=jnp.int32)
        matches = row_targets[:, None] == columns[None, :]
        local_target = jnp.sum(jnp.where(matches, logits, 0.0), axis=1)
        largest, expsum, target_sum = combined_all(
            (local_max, local_sum, local_target), "vert", combine
        )
        log_total = largest + jnp.log(expsum)
        return (logits - log_total[:, None], target_sum - log_total)

    first_row = lax.axis_index("ha") * own_rows
    gathered = lax.all_gather(hidden, "vert", axis=0, tiled=True)
    summed = lax.psum_scatter(
        partial_terms(lax.slice_in_dim(gathered, 0, own_rows * lax.axis_size("ha"), axis=0)).astype(
            jnp.bfloat16
        ),
        "ha",
        scatter_dimension=0,
        tiled=True,
    ).astype(jnp.float32)
    row_targets = lax.dynamic_slice_in_dim(targets, first_row, own_rows, 0)
    log_probs, picked = finish(summed, row_targets)
    return (log_probs, picked)


MESH = pl.DeviceIdType.MESH
CORES = 2
INNER = 2
LANES = 128
LOWEST = -3e38
GRANT = 60 * 1024 * 1024


def tiles_of(width, tile):
    return [(start, min(tile, width - start)) for start in range(0, width, tile)]


def kernel(
    sizes, hidden_ref, gain_ref, weight_ref, targets_ref, out_ref, level_ref, picked_ref,
    gathered, weight, total, turned, squares, stats, square_in, square_out, wanted, *rest
):
    outer, chunks, depth, batch, own_rows, tiles = sizes
    count = len(tiles)
    outgoing, incoming = rest[:count], rest[count : 2 * count]
    (own_sem, weight_sem, f_send, z_send, z_recv, y_send, y_recv, d_send, d_recv,
     x_send, x_recv, q_send, q_recv, s_send, s_recv) = rest[2 * count :]
    ha = lax.axis_index("ha")
    me = lax.axis_index("vert")
    vert = outer * INNER * CORES
    z, y, c = me // (INNER * CORES), (me // CORES) % INNER, me % CORES

    def at(zz, yy, cc):
        return (ha, (zz * INNER + yy) * CORES + cc)

    side = z // 2
    end, inner, far_inner = 3 * side, 1 + side, 2 - side
    partner = end + inner - z
    far_half = pl.ds(2 * (1 - side), 2)
    across = (1 - ha, me)
    beside = at(z, 1 - y, c)
    sibling = at(z, y, 1 - c)

    own_copies = [
        pltpu.make_async_copy(
            hidden_ref.at[:, pl.ds(k * depth, depth)], gathered.at[k, z, y, c], own_sem.at[k]
        )
        for k in range(chunks)
    ]
    for copy in own_copies:
        copy.start()
    weight_copies = [
        pltpu.make_async_copy(
            weight_ref.at[:, pl.ds(k * depth, depth)], weight.at[k], weight_sem.at[k]
        )
        for k in range(chunks)
    ]
    for copy in weight_copies[:AHEAD]:
        copy.start()

    barrier = pltpu.get_barrier_semaphore()
    for step in range(1, vert):
        pl.semaphore_signal(
            barrier, inc=1, device_id=(ha, (me + step) % vert), device_id_type=MESH
        )
    pl.semaphore_signal(barrier, inc=1, device_id=across, device_id_type=MESH)
    pl.semaphore_wait(barrier, vert)

    def remote(src, dst, send, recv, device):
        return pltpu.make_async_remote_copy(
            src_ref=src, dst_ref=dst, send_sem=send, recv_sem=recv,
            device_id=device, device_id_type=MESH,
        )

    for k in range(chunks):
        own_copies[k].wait()
        mine = gathered.at[k, z, y, c]
        for device in (at(far_inner, y, c), at(partner, y, c)):
            remote(mine, mine, z_send.at[k], z_recv.at[k], device).start()
        remote(mine, mine, y_send.at[k], y_recv.at[k], beside).start()

    wanted[...] = jnp.transpose(
        jnp.broadcast_to(targets_ref[...].astype(jnp.float32), (LANES, LANES))
    )
    total[...] = jnp.zeros_like(total)
    squares[...] = jnp.zeros_like(squares)

    def three(k, send, recv, device):
        block = gathered.at[k, pl.ds(0, outer - 1), 0, 0]
        return remote(block, block, send.at[k], recv.at[k], device)

    def two(k, send, recv, device):
        block = gathered.at[k, pl.ds(0, 2), 0, 0]
        return remote(block, block, send.at[k], recv.at[k], device)

    def four(k, send, recv, device):
        block = gathered.at[k, :, 0, 0]
        return remote(block, block, send.at[k], recv.at[k], device)

    def eight(k, send, recv, device):
        block = gathered.at[k, :, :, 0]
        return remote(block, block, send.at[k], recv.at[k], device)

    def relay(k):
        block = gathered.at[k, far_half, y, c]
        return remote(block, block, f_send.at[k], z_recv.at[k], at(end, y, c))

    def stage_a(k):
        three(k, z_send, z_recv, beside).wait_recv()

        @pl.when(z == inner)
        def _():
            relay(k).start()

        for step in range(1, outer):
            piece = gathered.at[k, (z + step) % outer, y, c]
            remote(piece, piece, y_send.at[k], y_recv.at[k], beside).start()
        column = gathered.at[k, :, y, c]
        remote(column, column, d_send.at[k], d_recv.at[k], sibling).start()

    def stage_b(k):
        four(k, y_send, y_recv, beside).wait_recv()
        column = gathered.at[k, :, 1 - y, c]
        remote(column, column, d_send.at[k], d_recv.at[k], sibling).start()

    def stage_c(k):
        eight(k, d_send, d_recv, sibling).wait_recv()
        pltpu.make_async_copy(
            weight_ref.at[:, pl.ds(pl.multiple_of(k * depth, depth), depth)],
            weight.at[k], weight_sem.at[k],
        ).wait()

        @pl.when(k + AHEAD < chunks)
        def _():
            later = k + AHEAD
            pltpu.make_async_copy(
                weight_ref.at[:, pl.ds(pl.multiple_of(later * depth, depth), depth)],
                weight.at[later], weight_sem.at[later],
            ).start()

        widened = gathered[k].astype(jnp.float32).reshape(batch, depth)
        squares[...] += sum(
            widened[:, lane : lane + LANES] * widened[:, lane : lane + LANES]
            for lane in range(0, depth, LANES)
        )
        gain = gain_ref[k]
        return (widened * gain).astype(jnp.bfloat16)

    def product(k, scaled, tile):
        start, width = tile
        return lax.dot_general(
            weight[k, pl.ds(start, width), :], scaled, (((1,), (1,)), ((), ())),
            preferred_element_type=jnp.float32,
        )

    stage_a(0)
    stage_a(1)
    stage_b(0)

    def body(k, carry):
        @pl.when(k + 2 < chunks)
        def _():
            stage_a(k + 2)

        stage_b(k + 1)
        scaled = stage_c(k)
        for tile in tiles:
            total[pl.ds(*tile), :] += product(k, scaled, tile)
        return carry

    lax.fori_loop(0, chunks - 1, body, 0)

    last = chunks - 1
    scaled = stage_c(last)
    kept = pl.ds(pl.multiple_of(ha * own_rows, own_rows), own_rows)
    given = pl.ds(pl.multiple_of((1 - ha) * own_rows, own_rows), own_rows)
    square_out[...] = squares[given, :]
    square_copy = remote(square_out, square_in, q_send.at[0], q_recv.at[0], across)
    square_copy.start()
    x_copies = []
    for j, tile in enumerate(tiles):
        total[pl.ds(*tile), :] += product(last, scaled, tile)
        padded = pl.ds(tile[0], TILE)
        turned[:, padded] = jnp.transpose(total[padded, :])
        outgoing[j][...] = turned[given, padded].astype(jnp.bfloat16)
        copy = remote(outgoing[j], incoming[j], x_send.at[j], x_recv.at[j], across)
        copy.start()
        x_copies.append(copy)

    square_copy.wait_recv()
    summed = jnp.sum(squares[kept, :] + square_in[...], axis=1, keepdims=True)
    inverse = lax.rsqrt(summed / D + 1e-05)
    vocab_width = out_ref.shape[1]
    base = me * vocab_width
    chosen = wanted[kept, 0:1].astype(jnp.int32) - base
    chosen = jnp.where(chosen < vocab_width, chosen, -1)
    lane = lax.broadcasted_iota(jnp.int32, (own_rows, LANES), 1)
    largest = jnp.full((own_rows, LANES), LOWEST, jnp.float32)
    expsum = jnp.zeros((own_rows, LANES), jnp.float32)
    target_sum = jnp.zeros((own_rows, LANES), jnp.float32)
    for j, (start, width) in enumerate(tiles):
        x_copies[j].wait_recv()
        padded = pl.ds(start, TILE)
        logits = (turned[kept, padded] + incoming[j][...].astype(jnp.float32)) * inverse
        out_ref[:, pl.ds(start, width)] = logits[:, :width]
        pieces = []
        for at_lane in range(0, width, LANES):
            piece = logits[:, at_lane : at_lane + LANES]
            left = width - at_lane
            if left < LANES:
                piece = jnp.where(lane < left, piece, LOWEST)
            pieces.append(piece)
            target_sum += jnp.where(lane + (start + at_lane) == chosen, piece, 0.0)
        raised = functools.reduce(jnp.maximum, pieces, largest)
        expsum = expsum * jnp.exp(largest - raised) + sum(
            jnp.exp(piece - raised) for piece in pieces
        )
        largest = raised
    row_max = jnp.max(largest, axis=1, keepdims=True)
    row_sum = jnp.sum(expsum * jnp.exp(largest - row_max), axis=1, keepdims=True)
    row_target = jnp.sum(target_sum, axis=1, keepdims=True)
    packed = jnp.where(lane == 0, row_max, jnp.where(lane == 1, row_sum, row_target))
    packed = jnp.concatenate([packed] * (LANES // own_rows), axis=0)
    turned_stats = jnp.transpose(packed)
    for part in range(3):
        stats[me, :, pl.ds(part * LANES, LANES)] = turned_stats[part : part + 1, :]
    copies = [
        remote(stats.at[me], stats.at[me], s_send, s_recv, (ha, (me + step) % vert))
        for step in range(1, vert)
    ]
    for copy in copies:
        copy.start()
    others = stats.at[pl.ds(0, vert - 1)]
    remote(others, others, s_send, s_recv, sibling).wait_recv()
    tops = stats[:, 0, pl.ds(0, LANES)]
    overall = jnp.max(tops, axis=0, keepdims=True)
    sums = jnp.sum(
        jnp.exp(tops - overall) * stats[:, 0, pl.ds(LANES, LANES)], axis=0, keepdims=True
    )
    log_total = overall + jnp.log(sums)
    picked = jnp.sum(stats[:, 0, pl.ds(2 * LANES, LANES)], axis=0, keepdims=True) - log_total
    picked_ref[...] = picked[:, :own_rows]
    level_ref[...] = jnp.transpose(jnp.broadcast_to(log_total, (LANES, LANES)))[:own_rows, :]

    remote(others, others, s_send, s_recv, sibling).wait_send()
    square_copy.wait_send()
    for copy in x_copies:
        copy.wait_send()

    def drain(k, carry):
        two(k, z_send, z_recv, beside).wait_send()

        @pl.when(z == inner)
        def _():
            relay(k).wait_send()

        four(k, y_send, y_recv, beside).wait_send()
        eight(k, d_send, d_recv, sibling).wait_send()
        return carry

    lax.fori_loop(0, chunks, drain, 0)


def finish(logits_ref, level_ref, picked_ref, out_ref, target_ref):
    out_ref[...] = logits_ref[...] - level_ref[:, 0:1]
    target_ref[...] = picked_ref[...]


def fused(hidden, norm_gain, head_weight, targets):
    rows, features = hidden.shape
    vocab_width = head_weight.shape[1]
    vert = lax.axis_size("vert")
    outer = vert // (INNER * CORES)
    batch = rows * vert
    own_rows = batch // lax.axis_size("ha")
    chunks = CHUNKS
    depth = features // chunks
    tiles = tiles_of(vocab_width, TILE)
    dma = pltpu.SemaphoreType.DMA
    hbm = pl.BlockSpec(memory_space=pltpu.HBM)
    vmem = pl.BlockSpec(memory_space=pltpu.VMEM)
    logits, level, picked = pl.pallas_call(
        functools.partial(kernel, (outer, chunks, depth, batch, own_rows, tiles)),
        out_shape=(
            jax.ShapeDtypeStruct((own_rows, vocab_width), jnp.float32),
            jax.ShapeDtypeStruct((own_rows, LANES), jnp.float32),
            jax.ShapeDtypeStruct((1, own_rows), jnp.float32),
        ),
        in_specs=[hbm, vmem, hbm, vmem],
        out_specs=(vmem, vmem, vmem),
        scratch_shapes=[
            pltpu.VMEM((chunks, outer, INNER, CORES, rows, depth), jnp.bfloat16),
            pltpu.VMEM((chunks, vocab_width, depth), jnp.bfloat16),
            pltpu.VMEM((TILE * len(tiles), batch), jnp.float32),
            pltpu.VMEM((batch, TILE * len(tiles)), jnp.float32),
            pltpu.VMEM((batch, LANES), jnp.float32),
            pltpu.VMEM((vert, 1, 3 * LANES), jnp.float32),
            pltpu.VMEM((own_rows, LANES), jnp.float32),
            pltpu.VMEM((own_rows, LANES), jnp.float32),
            pltpu.VMEM((batch, LANES), jnp.float32),
        ]
        + [pltpu.VMEM((own_rows, TILE), jnp.bfloat16) for _ in tiles] * 2
        + [dma((chunks,))] * 9
        + [dma((len(tiles),))] * 2
        + [dma((1,))] * 2
        + [dma(())] * 2,
        compiler_params=pltpu.CompilerParams(
            collective_id=0, has_side_effects=True, vmem_limit_bytes=GRANT
        ),
        name="head",
    )(hidden, norm_gain.reshape(chunks, 1, depth), head_weight.T, targets.reshape(1, batch))
    log_probs, target_logprob = pl.pallas_call(
        finish,
        out_shape=(
            jax.ShapeDtypeStruct((own_rows, vocab_width), jnp.float32),
            jax.ShapeDtypeStruct((1, own_rows), jnp.float32),
        ),
        in_specs=[vmem] * 3,
        out_specs=(vmem, vmem),
        name="finish",
    )(logits, level, picked)
    return log_probs, target_logprob.reshape(own_rows)


def local(hidden, norm_gain, head_weight, targets):
    rows, features = hidden.shape
    vert, ha = lax.axis_size("vert"), lax.axis_size("ha")
    own_rows = rows * vert // ha
    fits = (
        rows == 8
        and ha == 2
        and rows * vert == LANES
        and vert == 4 * INNER * CORES
        and features % (CHUNKS * LANES) == 0
        and head_weight.size * 2 <= 40 * 2**20
    )
    return (fused if fits else shards)(hidden, norm_gain, head_weight, targets)


CHUNKS = 4
AHEAD = 2
TILE = 512


def solution(mesh):
    placed = (P("vert", "ha"), P("ha"), P("ha", "vert"), P())
    return jax.shard_map(
        local, mesh=mesh, in_specs=placed, out_specs=(P("ha", "vert"), P("ha")), check_vma=False
    )
```
